256 devices in a mesh: ep: 32 (over x, z_hi, y), dp: 8 (over z_lo, core).
Axes of the slice: x: 4, y: 4, z: 8 (z_hi: 2, z_lo: 4; z = z_hi * 4 + z_lo), core: 2. Of those that a mesh axis runs over, the one named last changes fastest.
Arguments:
- master_weights: float32 [32, 1024, 3584], P('ep', 'dp'), may hold values from -6 to 6
- first_moment: float32 [32, 1024, 3584], P('ep', 'dp'), may hold values from -6 to 6
- second_moment: float32 [32, 1024, 3584], P('ep', 'dp'), may hold values from 0.01 to 4
- expert_ids: int32 [32], replicated, may hold values from 0 to 255, as said below
- bucket_offsets: int32 [1024], replicated, may hold values from 0 to 1023, as said below
- writer_rank: int32 [1024], replicated, may hold values from 0 to 7, as said below
Outputs:
- saved: bfloat16 [3, 32, 1024, 3584], P(None, 'ep', 'dp')
The draws below stay inside these ranges and needn't reach their ends.
Inputs may be any that keep to these rules, and one draw needn't show every extreme that they name: `expert_ids`: 32 different global expert numbers. `bucket_offsets`: each saved row named exactly once. `writer_rank`: of the bucket rows held by any one dp index, exactly 1024 // (8 * 8) are written by each dp index.
All inputs are finite; a program needn't handle non-finite values.
Results may differ from the reference program's by a relative error of at most 0.001.
Values may be sent and summed in bfloat16 or wider, within the bound.
A program may use at most 128 MiB of HBM per device.

```python
import math
import jax
import jax.numpy as jnp

ROWS = 1024
COLS = 3584
ALL_EXPERTS = 256
EXPERTS = 32
N_DP = 8


def layout_tables(key):
    shard_rows = ROWS // N_DP
    shuffle = jax.random.permutation(jax.random.fold_in(key, 11), ROWS).astype(jnp.int32)
    pattern = jnp.tile(jnp.arange(N_DP, dtype=jnp.int32), shard_rows // N_DP)
    shard_keys = jax.random.split(jax.random.fold_in(key, 12), N_DP)
    chosen = jax.vmap(lambda single: jax.random.permutation(single, pattern))(shard_keys).reshape(ROWS)
    writers = jnp.zeros((ROWS,), jnp.int32).at[shuffle].set(chosen.astype(jnp.int32))
    return (shuffle, writers)


def draw_expert_ids(key, part):
    return jax.random.permutation(jax.random.fold_in(key, 5), ALL_EXPERTS)[:EXPERTS].astype(jnp.int32)


def draw_bucket_offsets(key, part):
    return layout_tables(key)[0]


def draw_writer_rank(key, part):
    return layout_tables(key)[1]


def level_of(key, dims, cuts, least, high):
    level = 1.0
    for dim, parts in cuts:
        draws = jax.random.uniform(jax.random.fold_in(jax.random.fold_in(key, 6), dim), (parts,), jnp.float32, least / len(cuts), high / len(cuts))
        level = level * jnp.repeat(jnp.exp(draws), dims[dim] // parts).reshape((-1,) + (1,) * (len(dims) - 1 - dim))
    return level


def scatter_about(own_key, dims, spread, limit, shards=(), kind=jnp.bfloat16):
    drawn = spread * jax.random.normal(own_key, dims, jnp.float32)
    if shards:
        drawn = drawn * level_of(own_key, dims, shards, -0.22, 0.18)
    return jnp.clip(drawn, -limit, limit).astype(kind)


def setup_inputs(seed: int = 0) -> dict:
    streams_of = jax.random.split(jax.random.key(seed), 7)
    master_weights = scatter_about(streams_of[0], (EXPERTS, ROWS, COLS), 1.0, 6.0, ((0, 32), (1, 8)), jnp.float32)
    first_moment = scatter_about(streams_of[1], (EXPERTS, ROWS, COLS), 1.0, 6.0, ((0, 32), (1, 8)), jnp.float32)
    second_moment = jnp.clip(jnp.exp(math.log(4.0) - 5.9914646 * jax.random.uniform(streams_of[2], (EXPERTS, ROWS, COLS), jnp.float32) ** level_of(streams_of[2], (EXPERTS, ROWS, COLS), ((0, 32), (1, 8)), -0.2, 0.2)), 0.01, 4.0)
    expert_ids = draw_expert_ids(jax.random.fold_in(streams_of[6], 71), 0)
    bucket_offsets = draw_bucket_offsets(jax.random.fold_in(streams_of[6], 71), 0)
    writer_rank = draw_writer_rank(jax.random.fold_in(streams_of[6], 71), 0)
    return {"master_weights": master_weights, "first_moment": first_moment, "second_moment": second_moment, "expert_ids": expert_ids, "bucket_offsets": bucket_offsets, "writer_rank": writer_rank}


def destinations(bucket_offsets, writer_rank, shard_rows, groups):
    indicator = (writer_rank[:, None] == jnp.arange(groups, dtype=jnp.int32)[None, :]).astype(jnp.int32)
    before = jnp.cumsum(indicator, axis=0) - indicator
    within = jnp.sum(before * indicator, axis=1).astype(jnp.int32)
    placed = writer_rank * shard_rows + within
    return jnp.take(placed, bucket_offsets)


def reference(master_weights, first_moment, second_moment, expert_ids, bucket_offsets, writer_rank):
    target = destinations(bucket_offsets, writer_rank, ROWS // N_DP, N_DP)
    source_rows = jnp.argsort(target)
    source_order = jnp.argsort(expert_ids)

    def arrange(field):
        moved = jnp.take(field.astype(jnp.bfloat16), source_order, axis=0)
        return jnp.take(moved, source_rows, axis=1)

    return jnp.stack([arrange(master_weights), arrange(first_moment), arrange(second_moment)])
```

```python
import functools

import jax
import jax.numpy as jnp
import numpy as np
from jax import lax
from jax.experimental import pallas as pl
from jax.experimental.pallas import tpu as pltpu
from jax.sharding import PartitionSpec as P

MESH = pl.DeviceIdType.MESH
CHUNKS, SUB, WIDTH = 7, 2, 256
BLOCK = 24 * SUB
UNIT = 3 * SUB
BINS = ((0, 2), (3, 5), (6, 7), (8, 8), (9, 10), (11, 13), (14, 16))
BIN_OF = np.array([b for b, (lo, hi) in enumerate(BINS) for _ in range(lo, hi + 1)], np.int32)
XY = ((1, 0), (0, 1), (3, 0), (0, 3), (1, 1), (2, 0), (3, 3), (0, 2), (1, 3), (2, 1), (3, 1), (2, 2), (1, 2), (2, 3), (3, 2))
LAG = 2


def rows_for(n):
    return max(16, -(-UNIT * n // 16) * 16)


def one_hot_rows(slots, rows):
    width = slots.shape[1]
    at = lax.broadcasted_iota(jnp.int32, (rows, width), 0)
    return jnp.where(at == slots, 1.0, 0.0).astype(jnp.bfloat16)


def comm_kernel(
    same, other, slot1_ref, tab_ref, spread2_ref, stat2_ref, spread3_ref, stat3_ref, x0, x1, x2, out,
    xin, sel1, sel2, sel3, send_a, recv_a, send_s, recv_s, send_o, recv_o, send_b,
    in_sem, a_send, a_recv, s_send, s_recv, o_send, o_recv, b_send, b_recv, own_sem,
):
    ep, dp = lax.axis_index("ep"), lax.axis_index("dp")
    x, zh, y = ep // 8, (ep // 4) % 2, ep % 4
    zl, core = dp // 2, dp % 2
    me = x * 4 + y

    def xy_peer(dx, dy):
        px, py = (x + dx) % 4, (y + dy) % 4
        return px * 4 + py, (px * 8 + zh * 4 + py, dp)

    def dp_peer(dz, dc):
        return ((zl + dz) % 4) * 2 + (core + dc) % 2

    flipped = x * 8 + (1 - zh) * 4 + y
    same_offs = [(a, c) for a in (1, 3, 2) for c in (0, 1)] + [(0, 1)]
    other_offs = [(a, c) for a in (0, 1, 3, 2) for c in (0, 1)]

    for f, ref in enumerate((x0, x1, x2)):
        def load(c, carry, f=f, ref=ref):
            cols = pl.ds(pl.multiple_of(c * (SUB * WIDTH), SUB * WIDTH), SUB * WIDTH)
            pltpu.make_async_copy(ref.at[:, cols], xin.at[f, c], in_sem.at[f, c]).start()
            return carry
        lax.fori_loop(0, CHUNKS, load, 0)

    barrier = pltpu.get_barrier_semaphore()
    for dx, dy in XY:
        pl.semaphore_signal(barrier, inc=1, device_id=xy_peer(dx, dy)[1], device_id_type=MESH)
    for a, c in same_offs:
        pl.semaphore_signal(barrier, inc=1, device_id=(ep, dp_peer(a, c)), device_id_type=MESH)
    for a, c in other_offs:
        pl.semaphore_signal(barrier, inc=1, device_id=(flipped, dp_peer(a, c)), device_id_type=MESH)

    sel1[...] = one_hot_rows(slot1_ref[...], 128 * SUB)
    pl.semaphore_wait(barrier, len(XY) + len(same_offs) + len(other_offs))

    def stage1(c, carry):
        for f in range(3):
            pltpu.make_async_copy(x0.at[:, pl.ds(0, SUB * WIDTH)], xin.at[f, c], in_sem.at[f, c]).wait()
            rows = jnp.concatenate(
                [xin[f, c, :, h * WIDTH : (h + 1) * WIDTH].astype(jnp.bfloat16) for h in range(SUB)], axis=0
            )
            moved = jnp.dot(sel1[...], rows, preferred_element_type=jnp.float32).astype(jnp.bfloat16)
            send_a[c, :, f * 8 * SUB : (f + 1) * 8 * SUB, :] = moved.reshape(16, 8 * SUB, WIDTH)
        recv_a[c, me] = send_a[c, me]
        for dx, dy in XY:
            slot, dev = xy_peer(dx, dy)
            pltpu.make_async_remote_copy(
                send_a.at[c, slot], recv_a.at[c, me], a_send.at[c], a_recv.at[c], device_id=dev, device_id_type=MESH
            ).start()
        return carry

    lax.fori_loop(0, CHUNKS, stage1, 0)

    tab = tab_ref[...]
    look2 = jnp.dot(tab, spread2_ref[...], preferred_element_type=jnp.float32).astype(jnp.int32)
    sel2[...] = one_hot_rows(
        look2[1:2, :] + jnp.where(look2[2:3, :] > 0, stat2_ref[1:2, :], stat2_ref[0:1, :]), 8 * (same + other)
    )
    look3 = jnp.dot(tab, spread3_ref[...], preferred_element_type=jnp.float32).astype(jnp.int32)
    sel3[...] = one_hot_rows(look3[0:1, :] * BLOCK + stat3_ref[...], 16 * BLOCK)

    peer = xy_peer(1, 0)[1]

    def waiter(src, dst, send, recv):
        return pltpu.make_async_remote_copy(src, dst, send, recv, device_id=peer, device_id_type=MESH)

    def wait_a(c):
        return waiter(send_a.at[c, pl.ds(0, 15)], recv_a.at[c, pl.ds(0, 15)], a_send.at[c], a_recv.at[c])

    def wait_s(c):
        return waiter(send_s.at[c, pl.ds(0, 7)], recv_s.at[c, pl.ds(0, 7)], s_send.at[c], s_recv.at[c])

    def wait_o(c):
        return waiter(send_o.at[c], recv_o.at[c], o_send.at[c], o_recv.at[c])

    def wait_b(c):
        return waiter(send_b.at[c, pl.ds(0, 15)], out.at[c, pl.ds(0, 15)], b_send.at[c], b_recv.at[c])

    def stage2(c):
        wait_a(c).wait_recv()
        rows = recv_a[c].reshape(16 * BLOCK, WIDTH)
        moved = jnp.dot(sel2[...], rows, preferred_element_type=jnp.float32).astype(jnp.bfloat16)
        send_s[c] = moved[: 8 * same].reshape(8, same, WIDTH)
        send_o[c] = moved[8 * same :].reshape(8, other, WIDTH)
        recv_s[c, dp] = send_s[c, dp]
        for a, k in other_offs:
            to = dp_peer(a, k)
            pltpu.make_async_remote_copy(
                send_o.at[c, to], recv_o.at[c, dp], o_send.at[c], o_recv.at[c], device_id=(flipped, to), device_id_type=MESH
            ).start()
        for a, k in same_offs:
            to = dp_peer(a, k)
            pltpu.make_async_remote_copy(
                send_s.at[c, to], recv_s.at[c, dp], s_send.at[c], s_recv.at[c], device_id=(ep, to), device_id_type=MESH
            ).start()

    def stage3(c):
        wait_o(c).wait_recv()
        wait_s(c).wait_recv()
        rows = jnp.concatenate(
            [recv_s[c].reshape(8 * same, WIDTH), recv_o[c].reshape(8 * other, WIDTH)], axis=0
        )
        moved = jnp.dot(sel3[...], rows, preferred_element_type=jnp.float32).astype(jnp.bfloat16)
        send_b[c] = moved.reshape(16, BLOCK, WIDTH)
        pltpu.make_async_copy(send_b.at[c, me], out.at[c, me], own_sem.at[c]).start()
        for dx, dy in XY:
            slot, dev = xy_peer(dx, dy)
            pltpu.make_async_remote_copy(
                send_b.at[c, slot], out.at[c, me], b_send.at[c], b_recv.at[c], device_id=dev, device_id_type=MESH
            ).start()

    def step(s, carry):
        @pl.when(s < CHUNKS)
        def _():
            stage2(s)

        @pl.when(s >= LAG)
        def _():
            stage3(s - LAG)

        return carry

    lax.fori_loop(0, CHUNKS + LAG, step, 0)

    def finish(c, carry):
        wait_a(c).wait_send()
        wait_s(c).wait_send()
        wait_o(c).wait_send()
        wait_b(c).wait_send()
        wait_b(c).wait_recv()
        pltpu.make_async_copy(send_b.at[c, me], out.at[c, me], own_sem.at[c]).wait()
        return carry

    lax.fori_loop(0, CHUNKS, finish, 0)


def exchange(b, slot1, tab, x0, x1, x2):
    lo, hi = BINS[b]
    other, same = rows_for(hi), rows_for(16 - lo)
    total = 8 * (same + other)
    j, f, h, w = np.meshgrid(np.arange(16), np.arange(3), np.arange(SUB), np.arange(8), indexing="ij")
    j, f, h, w = (v.reshape(-1) for v in (j, f, h, w))
    spread2 = np.zeros((128, 16 * BLOCK), np.float32)
    spread2[j, np.arange(16 * BLOCK)] = 1.0
    stat2 = np.stack([w * same, 8 * same + w * other]) + f * SUB + h
    r = np.arange(total)
    far = r >= 8 * same
    cap = np.where(far, other, same)
    rr = np.where(far, r - 8 * same, r)
    p, rem = rr // cap, rr % cap
    k, f, h = rem // UNIT, (rem % UNIT) // SUB, rem % SUB
    real = k < 16
    spread3 = np.zeros((128, total), np.float32)
    spread3[np.where(real, far * 16 + k, 127), r] = 1.0
    stat3 = np.where(real, f * 8 * SUB + h * 8 + p, -1)[None]
    vm = pl.BlockSpec(memory_space=pltpu.VMEM)
    hbm = pl.BlockSpec(memory_space=pl.ANY)
    bf = jnp.bfloat16
    sems = [pltpu.SemaphoreType.DMA((3, CHUNKS))] + [pltpu.SemaphoreType.DMA((CHUNKS,))] * 9
    return pl.pallas_call(
        functools.partial(comm_kernel, same, other),
        out_shape=jax.ShapeDtypeStruct((CHUNKS, 16, BLOCK, WIDTH), bf),
        in_specs=[vm] * 6 + [hbm] * 3,
        out_specs=hbm,
        scratch_shapes=[
            pltpu.VMEM((3, CHUNKS, 128, SUB * WIDTH), jnp.float32),
            pltpu.VMEM((128 * SUB, 128 * SUB), bf),
            pltpu.VMEM((total, 16 * BLOCK), bf),
            pltpu.VMEM((16 * BLOCK, total), bf),
            pltpu.VMEM((CHUNKS, 16, BLOCK, WIDTH), bf),
            pltpu.VMEM((CHUNKS, 16, BLOCK, WIDTH), bf),
            pltpu.VMEM((CHUNKS, 8, same, WIDTH), bf),
            pltpu.VMEM((CHUNKS, 8, same, WIDTH), bf),
            pltpu.VMEM((CHUNKS, 8, other, WIDTH), bf),
            pltpu.VMEM((CHUNKS, 8, other, WIDTH), bf),
            pltpu.VMEM((CHUNKS, 16, BLOCK, WIDTH), bf),
            *sems,
        ],
        compiler_params=pltpu.CompilerParams(
            collective_id=b, has_side_effects=True, vmem_limit_bytes=60 * 1024 * 1024
        ),
        name=f"exchange_{b}",
    )(
        slot1, tab, jnp.asarray(spread2, bf), jnp.asarray(stat2, jnp.int32), jnp.asarray(spread3, bf),
        jnp.asarray(stat3, jnp.int32), x0, x1, x2,
    )


def place_kernel(slot_ref, rows_ref, out_ref):
    sel = one_hot_rows(slot_ref[...], 128 * SUB)
    for f in range(3):
        rows = rows_ref[0, :, f * 8 * SUB : (f + 1) * 8 * SUB, :].reshape(128 * SUB, WIDTH)
        moved = jnp.dot(sel, rows, preferred_element_type=jnp.float32).astype(jnp.bfloat16)
        for h in range(SUB):
            out_ref[f, :, h * WIDTH : (h + 1) * WIDTH] = moved[h * 128 : (h + 1) * 128]


def place(slot4, rows):
    return pl.pallas_call(
        place_kernel,
        grid=(CHUNKS,),
        out_shape=jax.ShapeDtypeStruct((3, 128, CHUNKS * SUB * WIDTH), jnp.bfloat16),
        in_specs=[
            pl.BlockSpec((1, 128 * SUB), lambda c: (0, 0)),
            pl.BlockSpec((1, 16, BLOCK, WIDTH), lambda c: (c, 0, 0, 0)),
        ],
        out_specs=pl.BlockSpec((3, 128, SUB * WIDTH), lambda c: (0, 0, c)),
        compiler_params=pltpu.CompilerParams(dimension_semantics=("arbitrary",)),
        name="place",
    )(slot4, rows)


def tables(expert_ids, bucket_offsets, writer_rank):
    i32 = jnp.int32
    ep, dp = lax.axis_index("ep"), lax.axis_index("dp")
    zh = (ep // 4) % 2
    e = jnp.arange(32, dtype=i32)
    plane = (e // 4) % 2
    pos = jnp.sum((expert_ids[None, :] < expert_ids[:, None]).astype(i32), axis=1)
    dz, dxy = (pos // 4) % 2, (pos // 8) * 4 + pos % 4
    ahead = (plane[None] == plane[:, None]) & (dz[None] == dz[:, None]) & (dxy[None] < dxy[:, None])
    k = jnp.sum(ahead.astype(i32), axis=1)
    m = jnp.sum(((plane == 0) & (dz == 1)).astype(i32))
    key = jnp.where(dz == zh, jnp.where(plane == zh, 0, 16) + k, -1)
    hit = key[None, :] == e[:, None]
    dtab = jnp.sum(jnp.where(hit, dxy[None, :] + 100, 0), axis=1) - 100
    j = jnp.arange(16, dtype=i32)
    mine = ((j // 4) * 8 + zh * 4 + j % 4)[:, None] == e[None, :]
    kj = jnp.sum(jnp.where(mine, k[None, :] * UNIT, 0), axis=1)
    oj = jnp.sum(jnp.where(mine, (dz != zh).astype(i32)[None, :], 0), axis=1)
    tab = jnp.zeros((8, 128), jnp.float32)
    tab = tab.at[0, :32].set(dtab.astype(jnp.float32)).at[1, :16].set(kj.astype(jnp.float32)).at[2, :16].set(oj.astype(jnp.float32))
    q = jnp.arange(1024, dtype=i32)
    within = jnp.sum(((writer_rank[None, :] == writer_rank[:, None]) & (q[None, :] < q[:, None])).astype(i32), axis=1)
    named = bucket_offsets[:, None] == q[None, :]
    both = jnp.sum(jnp.where(named, (writer_rank * 128 + within)[None, :], 0), axis=1)
    w, t = (both // 128).reshape(8, 128), (both % 128).reshape(8, 128)
    r = jnp.arange(128, dtype=i32)
    i = jnp.sum(((w[:, :, None] == w[:, None, :]) & (r[None, None, :] < r[None, :, None])).astype(i32), axis=2)
    slot = lax.dynamic_index_in_dim(i * (8 * SUB) + w, dp, 0, keepdims=True)
    slot1 = jnp.concatenate([slot + 8 * h for h in range(SUB)], axis=1)
    got = (w[None] == dp) & (i[None] == jnp.arange(16, dtype=i32)[:, None, None])
    t4 = jnp.sum(jnp.where(got, t[None], 0), axis=2)
    slot4 = (t4[:, None, :] + 128 * jnp.arange(SUB, dtype=i32)[None, :, None]).reshape(1, 128 * SUB)
    return m, tab.astype(jnp.bfloat16), slot1, slot4


def on_device(master_weights, first_moment, second_moment, expert_ids, bucket_offsets, writer_rank):
    m, tab, slot1, slot4 = tables(expert_ids, bucket_offsets, writer_rank)
    which = jnp.sum((m > jnp.asarray([hi for _, hi in BINS[:-1]], jnp.int32)).astype(jnp.int32))
    rows = lax.switch(
        which,
        [functools.partial(exchange, b) for b in range(len(BINS))],
        slot1, tab, master_weights[0], first_moment[0], second_moment[0],
    )
    return place(slot4, rows)[:, None]


def solution(mesh):
    return jax.shard_map(
        on_device,
        mesh=mesh,
        in_specs=(P("ep", "dp", None), P("ep", "dp", None), P("ep", "dp", None), P(), P(), P()),
        out_specs=P(None, "ep", "dp", None),
        check_vma=False,
    )
```

```python
import functools

import jax
import jax.numpy as jnp
import numpy as np
from jax import lax
from jax.experimental import pallas as pl
from jax.experimental.pallas import tpu as pltpu
from jax.sharding import PartitionSpec as P

MESH = pl.DeviceIdType.MESH
CHUNKS, SUB, WIDTH = 14, 2, 128
BLOCK = 24 * SUB
UNIT = 3 * SUB
BINS = ((0, 2), (3, 5), (6, 6), (7, 7), (8, 8), (9, 9), (10, 10), (11, 12), (13, 16))
XY = (
    (2, 2), (1, 2), (2, 1), (3, 2), (2, 3), (1, 1), (3, 3), (1, 3), (3, 1), (0, 2), (2, 0), (1, 0), (0, 1), (3, 0), (0, 3),
)
LEAD, LAG = 2, 2


def rows_for(n):
    return max(8, -(-UNIT * n // 8) * 8)


def one_hot_rows(slots, rows, start=0):
    at = start + lax.broadcasted_iota(jnp.int32, (rows, slots.shape[1]), 0)
    return jnp.where(at == slots, 1.0, 0.0).astype(jnp.bfloat16)


def fill_one_hot(ref, slots):
    def rows(b, carry):
        first = pl.multiple_of(b * 64, 64)
        ref[pl.ds(first, 64), :] = one_hot_rows(slots, 64, first)
        return carry

    lax.fori_loop(0, ref.shape[0] // 64, rows, 0)


def total_of(mask, value, axis):
    return jnp.sum(jnp.where(mask, value, 0.0), axis=axis, keepdims=True)


def counted(hot):
    earlier = lax.broadcasted_iota(jnp.int32, (128, 128), 0) < lax.broadcasted_iota(jnp.int32, (128, 128), 1)
    ones = jnp.where(hot, 1.0, 0.0).astype(jnp.bfloat16)
    return jnp.dot(ones, jnp.where(earlier, 1.0, 0.0).astype(jnp.bfloat16), preferred_element_type=jnp.float32)


def writers_and_places(writers):
    kind = lax.broadcasted_iota(jnp.int32, (8, 128), 0)
    carry = jnp.zeros((8, 1), jnp.float32)
    within = []
    for a in range(8):
        hot = writers[a : a + 1] == kind
        within.append(total_of(hot, counted(hot) + carry, 0))
        carry = carry + total_of(hot, 1.0, 1)
    return jnp.concatenate([writers.astype(jnp.float32), *within], axis=0).astype(jnp.bfloat16)


def row_facts(known, offsets):
    kind = lax.broadcasted_iota(jnp.int32, (8, 128), 0)
    found = jnp.dot(known, one_hot_rows(offsets % 128, 128), preferred_element_type=jnp.float32)
    row = kind == offsets // 128
    writer, place = total_of(row, found[:8], 0).astype(jnp.int32), total_of(row, found[8:], 0)
    hot = writer == kind
    return writer, place, total_of(hot, counted(hot), 0).astype(jnp.int32)


def landing(known, offsets_ref, dp):
    rows = lax.broadcasted_iota(jnp.int32, (128 * SUB, 128), 0)

    def shard(p, slots):
        writer, place, rank = row_facts(known, offsets_ref[pl.ds(p, 1), :])
        lane = jnp.where(writer == dp, rank * (8 * SUB) + p, -1024)
        hit = lane == rows
        for h in range(1, SUB):
            hit = hit | (lane + 8 * h == rows)
        return slots + lax.dot_general(
            jnp.broadcast_to(place, (8, 128)).astype(jnp.bfloat16), jnp.where(hit, 1.0, 0.0).astype(jnp.bfloat16),
            (((1,), (1,)), ((), ())), preferred_element_type=jnp.float32,
        )

    slots = lax.fori_loop(0, 8, shard, jnp.zeros((8, 128 * SUB), jnp.float32))
    part = (lax.broadcasted_iota(jnp.int32, (1, 128 * SUB), 1) // 8) % SUB
    return slots[0:1].astype(jnp.int32) + part * 128


def comm_kernel(
    same, other, offsets_ref, writers_ref, tab_ref, c2_ref, c3_ref, x0, x1, x2, out,
    xin, sel1, sel2, sel3, sel4, send_a, recv_a, send_s, recv_s, send_o, recv_o, send_b, recv_b,
    in_sem, a_send, a_recv, s_send, s_recv, o_send, o_recv, b_send, b_recv,
):
    ep, dp = lax.axis_index("ep"), lax.axis_index("dp")
    x, zh, y = ep // 8, (ep // 4) % 2, ep % 4
    zl, core = dp // 2, dp % 2
    me = x * 4 + y

    def xy_peer(dx, dy):
        px, py = (x + dx) % 4, (y + dy) % 4
        return px * 4 + py, (px * 8 + zh * 4 + py, dp)

    def dp_peer(dz, dc):
        return ((zl + dz) % 4) * 2 + (core + dc) % 2

    flipped = x * 8 + (1 - zh) * 4 + y
    same_offs = [(a, c) for a in (1, 3, 2) for c in (0, 1)] + [(0, 1)]
    other_offs = [(a, c) for a in (0, 1, 3, 2) for c in (0, 1)]

    barrier = pltpu.get_barrier_semaphore()
    for dx, dy in XY:
        pl.semaphore_signal(barrier, inc=1, device_id=xy_peer(dx, dy)[1], device_id_type=MESH)
    for a, c in same_offs:
        pl.semaphore_signal(barrier, inc=1, device_id=(ep, dp_peer(a, c)), device_id_type=MESH)
    for a, c in other_offs:
        pl.semaphore_signal(barrier, inc=1, device_id=(flipped, dp_peer(a, c)), device_id_type=MESH)

    def load(c, carry):
        cols = pl.ds(pl.multiple_of(c * (SUB * WIDTH), SUB * WIDTH), SUB * WIDTH)
        for f, ref in enumerate((x0, x1, x2)):
            pltpu.make_async_copy(ref.at[:, cols], xin.at[f, c], in_sem.at[f, c]).start()
        return carry

    lax.fori_loop(0, CHUNKS, load, 0)
    known = writers_and_places(writers_ref[...])
    writer, _, rank = row_facts(known, offsets_ref[pl.ds(dp, 1), :])
    slot = rank * (8 * SUB) + writer
    sel1[...] = one_hot_rows(jnp.concatenate([slot + 8 * h for h in range(SUB)], axis=1), 128 * SUB)

    def stage1(c):
        for f in range(3):
            pltpu.make_async_copy(x0.at[:, pl.ds(0, SUB * WIDTH)], xin.at[f, c], in_sem.at[f, c]).wait()
            rows = jnp.concatenate(
                [xin[f, c, :, h * WIDTH : (h + 1) * WIDTH].astype(jnp.bfloat16) for h in range(SUB)], axis=0
            )
            moved = jnp.dot(sel1[...], rows, preferred_element_type=jnp.float32).astype(jnp.bfloat16)
            send_a[c, :, f * 8 * SUB : (f + 1) * 8 * SUB, :] = moved.reshape(16, 8 * SUB, WIDTH)
        recv_a[c, me] = send_a[c, me]

    def start_a(c):
        for dx, dy in XY:
            slot, dev = xy_peer(dx, dy)
            pltpu.make_async_remote_copy(
                send_a.at[c, slot], recv_a.at[c, me], a_send.at[c], a_recv.at[c], device_id=dev, device_id_type=MESH
            ).start()

    peer = xy_peer(1, 0)[1]

    def waiter(src, dst, send, recv):
        return pltpu.make_async_remote_copy(src, dst, send, recv, device_id=peer, device_id_type=MESH)

    def wait_a(c):
        return waiter(send_a.at[c, pl.ds(0, 15)], recv_a.at[c, pl.ds(0, 15)], a_send.at[c], a_recv.at[c])

    def wait_s(c):
        return waiter(send_s.at[c, pl.ds(0, 7)], recv_s.at[c, pl.ds(0, 7)], s_send.at[c], s_recv.at[c])

    def wait_o(c):
        return waiter(send_o.at[c], recv_o.at[c], o_send.at[c], o_recv.at[c])

    def wait_b(c):
        return waiter(send_b.at[c, pl.ds(0, 15)], recv_b.at[c, pl.ds(0, 15)], b_send.at[c], b_recv.at[c])

    def stage2(c):
        wait_a(c).wait_recv()
        rows = recv_a[c].reshape(16 * BLOCK, WIDTH)
        moved = jnp.dot(sel2[...], rows, preferred_element_type=jnp.float32)
        send_o[c] = moved[8 * same :].reshape(8, other // 8, 8, WIDTH).astype(jnp.bfloat16)
        send_s[c] = moved[: 8 * same].reshape(8, same // 8, 8, WIDTH).astype(jnp.bfloat16)
        recv_s[c, dp] = send_s[c, dp]
        for a, k in other_offs:
            to = dp_peer(a, k)
            pltpu.make_async_remote_copy(
                send_o.at[c, to], recv_o.at[c, dp], o_send.at[c], o_recv.at[c], device_id=(flipped, to), device_id_type=MESH
            ).start()
        for a, k in same_offs:
            to = dp_peer(a, k)
            pltpu.make_async_remote_copy(
                send_s.at[c, to], recv_s.at[c, dp], s_send.at[c], s_recv.at[c], device_id=(ep, to), device_id_type=MESH
            ).start()

    def stage3(c):
        wait_o(c).wait_recv()
        wait_s(c).wait_recv()
        rows = jnp.concatenate(
            [
                recv_s[c].astype(jnp.float32).reshape(8 * same, WIDTH),
                recv_o[c].astype(jnp.float32).reshape(8 * other, WIDTH),
            ],
            axis=0,
        ).astype(jnp.bfloat16)
        moved = jnp.dot(sel3[...], rows, preferred_element_type=jnp.float32).astype(jnp.bfloat16)
        send_b[c] = moved.reshape(16, BLOCK, WIDTH)
        recv_b[c, me] = send_b[c, me]
        for dx, dy in XY:
            slot, dev = xy_peer(dx, dy)
            pltpu.make_async_remote_copy(
                send_b.at[c, slot], recv_b.at[c, me], b_send.at[c], b_recv.at[c], device_id=dev, device_id_type=MESH
            ).start()

    def stage4(c):
        wait_b(c).wait_recv()
        for f in range(3):
            rows = recv_b[c, :, f * 8 * SUB : (f + 1) * 8 * SUB, :].reshape(128 * SUB, WIDTH)
            moved = jnp.dot(sel4[...], rows, preferred_element_type=jnp.float32).astype(jnp.bfloat16)
            for h in range(SUB):
                cols = pl.ds(pl.multiple_of((c * SUB + h) * WIDTH, WIDTH), WIDTH)
                out[f, :, cols] = moved[h * 128 : (h + 1) * 128]

    stage1(0)
    pl.semaphore_wait(barrier, len(XY) + len(same_offs) + len(other_offs))
    start_a(0)

    def ahead(c, carry):
        stage1(c)
        start_a(c)
        return carry

    lax.fori_loop(1, LEAD, ahead, 0)
    tab = tab_ref[...].astype(jnp.bfloat16)
    look2 = jnp.dot(tab, one_hot_rows(c2_ref[0:1, :], 128), preferred_element_type=jnp.float32).astype(jnp.int32)
    fill_one_hot(sel2, look2[1:2, :] + jnp.where(look2[2:3, :] > 0, c2_ref[2:3, :], c2_ref[1:2, :]))
    look3 = jnp.dot(tab, one_hot_rows(c3_ref[0:1, :], 128), preferred_element_type=jnp.float32).astype(jnp.int32)
    fill_one_hot(sel3, look3[0:1, :] * BLOCK + c3_ref[1:2, :])
    sel4[...] = one_hot_rows(landing(known, offsets_ref, dp), 128 * SUB)

    def step(s, carry):
        @pl.when(s + LEAD < CHUNKS)
        def _():
            stage1(s + LEAD)
            start_a(s + LEAD)

        @pl.when(s < CHUNKS)
        def _():
            stage2(s)

        @pl.when((s >= LAG) & (s < CHUNKS + LAG))
        def _():
            stage3(s - LAG)

        @pl.when(s >= 2 * LAG)
        def _():
            stage4(s - 2 * LAG)

        return carry

    lax.fori_loop(0, CHUNKS + 2 * LAG, step, 0)

    def finish(c, carry):
        wait_a(c).wait_send()
        wait_s(c).wait_send()
        wait_o(c).wait_send()
        wait_b(c).wait_send()
        return carry

    lax.fori_loop(0, CHUNKS, finish, 0)


def exchange(b, offsets, writers, tab, x0, x1, x2):
    lo, hi = BINS[b]
    other, same = rows_for(hi), rows_for(16 - lo)
    total = 8 * (same + other)
    j, f, h, w = np.meshgrid(np.arange(16), np.arange(3), np.arange(SUB), np.arange(8), indexing="ij")
    j, f, h, w = (v.reshape(-1) for v in (j, f, h, w))
    c2 = np.stack([j, w * same + f * SUB + h, 8 * same + w * other + f * SUB + h])
    r = np.arange(total)
    far = r >= 8 * same
    cap = np.where(far, other, same)
    rr = np.where(far, r - 8 * same, r)
    p, rem = rr // cap, rr % cap
    k, f, h = rem // UNIT, (rem % UNIT) // SUB, rem % SUB
    real = k < 16
    c3 = np.stack([np.where(real, far * 16 + k, 127), np.where(real, f * 8 * SUB + h * 8 + p, -1)])
    vm = pl.BlockSpec(memory_space=pltpu.VMEM)
    hbm = pl.BlockSpec(memory_space=pl.ANY)
    bf = jnp.bfloat16
    blocks = pltpu.VMEM((CHUNKS, 16, BLOCK, WIDTH), bf)
    sems = [pltpu.SemaphoreType.DMA((3, CHUNKS))] + [pltpu.SemaphoreType.DMA((CHUNKS,))] * 8
    return pl.pallas_call(
        functools.partial(comm_kernel, same, other),
        out_shape=jax.ShapeDtypeStruct((3, 128, CHUNKS * SUB * WIDTH), bf),
        in_specs=[vm] * 5 + [hbm] * 3,
        out_specs=vm,
        scratch_shapes=[
            pltpu.VMEM((3, CHUNKS, 128, SUB * WIDTH), jnp.float32),
            pltpu.VMEM((128 * SUB, 128 * SUB), bf),
            pltpu.VMEM((total, 16 * BLOCK), bf),
            pltpu.VMEM((16 * BLOCK, total), bf),
            pltpu.VMEM((128 * SUB, 128 * SUB), bf),
            blocks,
            blocks,
            pltpu.VMEM((CHUNKS, 8, same // 8, 8, WIDTH), bf),
            pltpu.VMEM((CHUNKS, 8, same // 8, 8, WIDTH), bf),
            pltpu.VMEM((CHUNKS, 8, other // 8, 8, WIDTH), bf),
            pltpu.VMEM((CHUNKS, 8, other // 8, 8, WIDTH), bf),
            blocks,
            blocks,
            *sems,
        ],
        compiler_params=pltpu.CompilerParams(
            collective_id=b, has_side_effects=True, vmem_limit_bytes=56 * 1024 * 1024
        ),
        name=f"exchange_{b}",
    )(offsets, writers, tab, jnp.asarray(c2, jnp.int32), jnp.asarray(c3, jnp.int32), x0, x1, x2)


def tables_kernel(ids_ref, which_ref, tab_ref):
    i32, f32 = jnp.int32, jnp.float32
    zh = (lax.axis_index("ep") // 4) % 2

    def at(shape, d):
        return lax.broadcasted_iota(i32, shape, d)

    add = total_of
    eye = at((32, 32), 0) == at((32, 32), 1)

    def col(v):
        return add(eye, v.astype(f32), 1).astype(i32)

    ids, e = ids_ref[...], at((1, 32), 1)
    pos = add(col(ids) < ids, 1.0, 0).astype(i32)
    plane, dz, dxy = (e // 4) % 2, (pos // 4) % 2, (pos // 8) * 4 + pos % 4
    group = (plane * 2 + dz) * 16
    cg, cd = col(group), col(dxy)
    k = add((cg == group) & (cd < dxy), 1.0, 0).astype(i32)
    key = jnp.where(dz == zh, jnp.where(plane == zh, 0, 16) + k, -1)
    lane = at((32, 128), 1)
    dtab = add(col(key) == lane, (cd + 100).astype(f32), 0) - 100.0
    own = (at((32, 128), 0) == (lane // 4) * 8 + zh * 4 + lane % 4) & (lane < 16)
    kj = add(own, (col(k) * UNIT).astype(f32), 0)
    oj = add(own & (col(dz) != zh), 1.0, 0)
    r = at((8, 128), 0)
    tab_ref[...] = jnp.where(r == 0, dtab, jnp.where(r == 1, kj, jnp.where(r == 2, oj, 0.0)))
    m = jnp.sum(jnp.where((plane == 0) & (dz == 1), 1.0, 0.0)).astype(i32)
    which = jnp.int32(0)
    for _, hi in BINS[:-1]:
        which = which + jnp.where(m > hi, 1, 0)
    which_ref[0, 0] = which


def tables(expert_ids):
    vm = pl.BlockSpec(memory_space=pltpu.VMEM)
    return pl.pallas_call(
        tables_kernel,
        out_shape=(jax.ShapeDtypeStruct((1, 1), jnp.int32), jax.ShapeDtypeStruct((8, 128), jnp.float32)),
        in_specs=[vm],
        out_specs=(pl.BlockSpec(memory_space=pltpu.SMEM), vm),
        name="tables",
    )(expert_ids.reshape(1, 32))


def on_device(master_weights, first_moment, second_moment, expert_ids, bucket_offsets, writer_rank):
    which, tab = tables(expert_ids)
    saved = lax.switch(
        which[0, 0],
        [functools.partial(exchange, b) for b in range(len(BINS))],
        bucket_offsets.reshape(8, 128), writer_rank.reshape(8, 128), tab, master_weights[0], first_moment[0], second_moment[0],
    )
    return saved[:, None]


def solution(mesh):
    return jax.shard_map(
        on_device,
        mesh=mesh,
        in_specs=(P("ep", "dp", None), P("ep", "dp", None), P("ep", "dp", None), P(), P(), P()),
        out_specs=P(None, "ep", "dp", None),
        check_vma=False,
    )
```

```python
import functools

import jax
import jax.numpy as jnp
import numpy as np
from jax import lax
from jax.experimental import pallas as pl
from jax.experimental.pallas import tpu as pltpu
from jax.sharding import PartitionSpec as P

MESH = pl.DeviceIdType.MESH
CHUNKS, SUB, WIDTH = 14, 2, 128
BLOCK = 24 * SUB
UNIT = 3 * SUB
BINS = ((0, 2), (3, 5), (6, 6), (7, 7), (8, 8), (9, 9), (10, 10), (11, 12), (13, 16))
XY = (
    (2, 2), (1, 2), (2, 1), (3, 2), (2, 3), (1, 1), (3, 3), (1, 3), (3, 1), (0, 2), (2, 0), (1, 0), (0, 1), (3, 0), (0, 3),
)
ZC = tuple((1, a, c) for a in (0, 1, 3, 2) for c in (0, 1)) + tuple((0, a, c) for a in (1, 3, 2) for c in (0, 1)) + ((0, 0, 1),)
LEAD, LAG = 2, 2


def rows_for(n):
    return max(8, -(-UNIT * n // 8) * 8)


def one_hot_rows(slots, rows, start=0):
    at = start + lax.broadcasted_iota(jnp.int32, (rows, slots.shape[1]), 0)
    return jnp.where(at == slots, 1.0, 0.0).astype(jnp.bfloat16)


def fill_one_hot(ref, slots):
    def rows(b, carry):
        first = pl.multiple_of(b * 64, 64)
        ref[pl.ds(first, 64), :] = one_hot_rows(slots, 64, first)
        return carry

    lax.fori_loop(0, ref.shape[0] // 64, rows, 0)


def total_of(mask, value, axis):
    return jnp.sum(jnp.where(mask, value, 0.0), axis=axis, keepdims=True)


def side_by_side(v):
    return jnp.concatenate([v[8 * a : 8 * (a + 1)] for a in range(8)], axis=1)


def counted(hot):
    earlier = lax.broadcasted_iota(jnp.int32, (128, 128), 0) < lax.broadcasted_iota(jnp.int32, (128, 128), 1)
    ones = jnp.where(hot, 1.0, 0.0)
    ones = jnp.concatenate([ones[:, 128 * a : 128 * (a + 1)] for a in range(8)], axis=0).astype(jnp.bfloat16)
    return side_by_side(jnp.dot(ones, jnp.where(earlier, 1.0, 0.0).astype(jnp.bfloat16), preferred_element_type=jnp.float32))


def in_lanes(v):
    return jnp.concatenate([v[a : a + 1] for a in range(8)], axis=1)


def row_facts(writers, offsets):
    kind = lax.broadcasted_iota(jnp.int32, (8, 1024), 0)
    hot = in_lanes(writers) == kind
    count = counted(hot)
    carry = jnp.zeros((8, 1), jnp.float32)
    within = []
    for a in range(8):
        here = slice(128 * a, 128 * (a + 1))
        within.append(total_of(hot[:, here], count[:, here] + carry, 0))
        carry = carry + total_of(hot[:, here], 1.0, 1)
    known = jnp.concatenate([writers.astype(jnp.float32), *within], axis=0).astype(jnp.bfloat16)
    lanes = in_lanes(offsets)
    found = jnp.dot(known, one_hot_rows(lanes % 128, 128), preferred_element_type=jnp.float32)
    row = kind == lanes // 128
    writer, place = total_of(row, found[:8], 0).astype(jnp.int32), total_of(row, found[8:], 0)
    hot = writer == kind
    return writer, place, total_of(hot, counted(hot), 0).astype(jnp.int32)


def landing(writer, place, rank, dp):
    shard = lax.broadcasted_iota(jnp.int32, (1, 1024), 1) // 128
    rows = lax.broadcasted_iota(jnp.int32, (128 * SUB, 1024), 0)
    lane = jnp.where(writer == dp, rank * (8 * SUB) + shard, -1024)
    hit = lane == rows
    for h in range(1, SUB):
        hit = hit | (lane + 8 * h == rows)
    slots = lax.dot_general(
        jnp.broadcast_to(place, (8, 1024)).astype(jnp.bfloat16), jnp.where(hit, 1.0, 0.0).astype(jnp.bfloat16),
        (((1,), (1,)), ((), ())), preferred_element_type=jnp.float32,
    )
    part = (lax.broadcasted_iota(jnp.int32, (1, 128 * SUB), 1) // 8) % SUB
    return slots[0:1].astype(jnp.int32) + part * 128


def comm_kernel(
    same, other, offsets_ref, writers_ref, tab_ref, c2_ref, c3_ref, x0, x1, x2, out,
    held, xin, sel1, sel2, sel3, sel4, send_a, recv_a, send_s, recv_s, send_o, recv_o, send_b, recv_b,
    in_sem, a_send, a_recv, s_send, s_recv, o_send, o_recv, b_send, b_recv,
):
    ep, dp = lax.axis_index("ep"), lax.axis_index("dp")
    x, zh, y = ep // 8, (ep // 4) % 2, ep % 4
    zl, core = dp // 2, dp % 2
    me = x * 4 + y

    def xy_peer(dx, dy):
        px, py = (x + dx) % 4, (y + dy) % 4
        return px * 4 + py, (px * 8 + zh * 4 + py, dp)

    def dp_peer(dz, dc):
        return ((zl + dz) % 4) * 2 + (core + dc) % 2

    flipped = x * 8 + (1 - zh) * 4 + y
    same_offs = [(a, c) for far, a, c in ZC if not far]
    other_offs = [(a, c) for far, a, c in ZC if far]

    barrier = pltpu.get_barrier_semaphore()
    for dx, dy in XY:
        pl.semaphore_signal(barrier, inc=1, device_id=xy_peer(dx, dy)[1], device_id_type=MESH)
    for a, c in same_offs:
        pl.semaphore_signal(barrier, inc=1, device_id=(ep, dp_peer(a, c)), device_id_type=MESH)
    for a, c in other_offs:
        pl.semaphore_signal(barrier, inc=1, device_id=(flipped, dp_peer(a, c)), device_id_type=MESH)

    def load(c, carry):
        cols = pl.ds(pl.multiple_of(c * (SUB * WIDTH), SUB * WIDTH), SUB * WIDTH)
        for f, ref in enumerate((x0, x1, x2)):
            pltpu.make_async_copy(ref.at[:, cols], xin.at[f, c], in_sem.at[f, c]).start()
        return carry

    lax.fori_loop(0, CHUNKS, load, 0)
    writer, place, rank = row_facts(writers_ref[...], offsets_ref[...])
    for p in range(8):
        held[p : p + 1, :] = (rank * (8 * SUB) + writer)[:, 128 * p : 128 * (p + 1)]
    slot = held[pl.ds(dp, 1), :]
    sel1[...] = one_hot_rows(jnp.concatenate([slot + 8 * h for h in range(SUB)], axis=1), 128 * SUB)

    def stage1(c):
        for f in range(3):
            pltpu.make_async_copy(x0.at[:, pl.ds(0, SUB * WIDTH)], xin.at[f, c], in_sem.at[f, c]).wait()
            rows = jnp.concatenate(
                [xin[f, c, :, h * WIDTH : (h + 1) * WIDTH].astype(jnp.bfloat16) for h in range(SUB)], axis=0
            )
            moved = jnp.dot(sel1[...], rows, preferred_element_type=jnp.float32).astype(jnp.bfloat16)
            send_a[c, :, f * 8 * SUB : (f + 1) * 8 * SUB, :] = moved.reshape(16, 8 * SUB, WIDTH)
        recv_a[c, me] = send_a[c, me]

    def start_a(c):
        for dx, dy in XY:
            slot, dev = xy_peer(dx, dy)
            pltpu.make_async_remote_copy(
                send_a.at[c, slot], recv_a.at[c, me], a_send.at[c], a_recv.at[c], device_id=dev, device_id_type=MESH
            ).start()

    peer = xy_peer(1, 0)[1]

    def waiter(src, dst, send, recv):
        return pltpu.make_async_remote_copy(src, dst, send, recv, device_id=peer, device_id_type=MESH)

    def wait_a(c):
        return waiter(send_a.at[c, pl.ds(0, 15)], recv_a.at[c, pl.ds(0, 15)], a_send.at[c], a_recv.at[c])

    def wait_s(c):
        return waiter(send_s.at[c, pl.ds(0, 7)], recv_s.at[c, pl.ds(0, 7)], s_send.at[c], s_recv.at[c])

    def wait_o(c):
        return waiter(send_o.at[c], recv_o.at[c], o_send.at[c], o_recv.at[c])

    def wait_b(c):
        return waiter(send_b.at[c, pl.ds(0, 15)], recv_b.at[c, pl.ds(0, 15)], b_send.at[c], b_recv.at[c])

    def stage2(c):
        wait_a(c).wait_recv()
        rows = recv_a[c].reshape(16 * BLOCK, WIDTH)
        moved = jnp.dot(sel2[...], rows, preferred_element_type=jnp.float32)
        send_o[c] = moved[8 * same :].reshape(8, other // 8, 8, WIDTH).astype(jnp.bfloat16)
        send_s[c] = moved[: 8 * same].reshape(8, same // 8, 8, WIDTH).astype(jnp.bfloat16)
        recv_s[c, dp] = send_s[c, dp]
        for far, a, k in ZC:
            to = dp_peer(a, k)
            if far:
                src, dst, sems, at = send_o, recv_o, (o_send.at[c], o_recv.at[c]), flipped
            else:
                src, dst, sems, at = send_s, recv_s, (s_send.at[c], s_recv.at[c]), ep
            pltpu.make_async_remote_copy(
                src.at[c, to], dst.at[c, dp], *sems, device_id=(at, to), device_id_type=MESH
            ).start()

    def stage3(c):
        wait_o(c).wait_recv()
        wait_s(c).wait_recv()
        rows = jnp.concatenate(
            [
                recv_s[c].astype(jnp.float32).reshape(8 * same, WIDTH),
                recv_o[c].astype(jnp.float32).reshape(8 * other, WIDTH),
            ],
            axis=0,
        ).astype(jnp.bfloat16)
        moved = jnp.dot(sel3[...], rows, preferred_element_type=jnp.float32).astype(jnp.bfloat16)
        send_b[c] = moved.reshape(16, BLOCK, WIDTH)
        recv_b[c, me] = send_b[c, me]
        for dx, dy in XY:
            slot, dev = xy_peer(dx, dy)
            pltpu.make_async_remote_copy(
                send_b.at[c, slot], recv_b.at[c, me], b_send.at[c], b_recv.at[c], device_id=dev, device_id_type=MESH
            ).start()

    def stage4(c):
        wait_a(c).wait_send()
        wait_s(c).wait_send()
        wait_o(c).wait_send()
        wait_b(c).wait_recv()
        for f in range(3):
            rows = recv_b[c, :, f * 8 * SUB : (f + 1) * 8 * SUB, :].reshape(128 * SUB, WIDTH)
            moved = jnp.dot(sel4[...], rows, preferred_element_type=jnp.float32).astype(jnp.bfloat16)
            for h in range(SUB):
                cols = pl.ds(pl.multiple_of((c * SUB + h) * WIDTH, WIDTH), WIDTH)
                out[f, :, cols] = moved[h * 128 : (h + 1) * 128]

    stage1(0)
    pl.semaphore_wait(barrier, len(XY) + len(same_offs) + len(other_offs))
    start_a(0)

    tab = tab_ref[...].astype(jnp.bfloat16)
    look2 = jnp.dot(tab, one_hot_rows(c2_ref[0:1, :], 128), preferred_element_type=jnp.float32).astype(jnp.int32)
    fill_one_hot(sel2, look2[1:2, :] + jnp.where(look2[2:3, :] > 0, c2_ref[2:3, :], c2_ref[1:2, :]))

    sel4[...] = one_hot_rows(landing(writer, place, rank, dp), 128 * SUB)

    def ahead(c, carry):
        stage1(c)
        start_a(c)
        return carry

    lax.fori_loop(1, LEAD, ahead, 0)
    def late_tables():
        look3 = jnp.dot(tab, one_hot_rows(c3_ref[0:1, :], 128), preferred_element_type=jnp.float32).astype(jnp.int32)
        fill_one_hot(sel3, look3[0:1, :] * BLOCK + c3_ref[1:2, :])

    def step(s, carry):
        @pl.when(s + LEAD < CHUNKS)
        def _():
            stage1(s + LEAD)
            start_a(s + LEAD)

        @pl.when(s < CHUNKS)
        def _():
            stage2(s)

        pl.when(s == 1)(late_tables)

        @pl.when((s >= LAG) & (s < CHUNKS + LAG))
        def _():
            stage3(s - LAG)

        @pl.when(s >= 2 * LAG)
        def _():
            stage4(s - 2 * LAG)

        return carry

    lax.fori_loop(0, CHUNKS + 2 * LAG, step, 0)

    def finish(c, carry):
        wait_b(c).wait_send()
        return carry

    lax.fori_loop(0, CHUNKS, finish, 0)


def exchange(b, offsets, writers, tab, x0, x1, x2):
    lo, hi = BINS[b]
    other, same = rows_for(hi), rows_for(16 - lo)
    total = 8 * (same + other)
    j, f, h, w = np.meshgrid(np.arange(16), np.arange(3), np.arange(SUB), np.arange(8), indexing="ij")
    j, f, h, w = (v.reshape(-1) for v in (j, f, h, w))
    c2 = np.stack([j, w * same + f * SUB + h, 8 * same + w * other + f * SUB + h])
    r = np.arange(total)
    far = r >= 8 * same
    cap = np.where(far, other, same)
    rr = np.where(far, r - 8 * same, r)
    p, rem = rr // cap, rr % cap
    k, f, h = rem // UNIT, (rem % UNIT) // SUB, rem % SUB
    real = k < 16
    c3 = np.stack([np.where(real, far * 16 + k, 127), np.where(real, f * 8 * SUB + h * 8 + p, -1)])
    vm = pl.BlockSpec(memory_space=pltpu.VMEM)
    hbm = pl.BlockSpec(memory_space=pl.ANY)
    bf = jnp.bfloat16
    blocks = pltpu.VMEM((CHUNKS, 16, BLOCK, WIDTH), bf)
    sems = [pltpu.SemaphoreType.DMA((3, CHUNKS))] + [pltpu.SemaphoreType.DMA((CHUNKS,))] * 8
    return pl.pallas_call(
        functools.partial(comm_kernel, same, other),
        out_shape=jax.ShapeDtypeStruct((3, 128, CHUNKS * SUB * WIDTH), bf),
        in_specs=[vm] * 5 + [hbm] * 3,
        out_specs=vm,
        scratch_shapes=[
            pltpu.VMEM((8, 128), jnp.int32),
            pltpu.VMEM((3, CHUNKS, 128, SUB * WIDTH), jnp.float32),
            pltpu.VMEM((128 * SUB, 128 * SUB), bf),
            pltpu.VMEM((total, 16 * BLOCK), bf),
            pltpu.VMEM((16 * BLOCK, total), bf),
            pltpu.VMEM((128 * SUB, 128 * SUB), bf),
            blocks,
            blocks,
            pltpu.VMEM((CHUNKS, 8, same // 8, 8, WIDTH), bf),
            pltpu.VMEM((CHUNKS, 8, same // 8, 8, WIDTH), bf),
            pltpu.VMEM((CHUNKS, 8, other // 8, 8, WIDTH), bf),
            pltpu.VMEM((CHUNKS, 8, other // 8, 8, WIDTH), bf),
            blocks,
            blocks,
            *sems,
        ],
        compiler_params=pltpu.CompilerParams(
            collective_id=b, has_side_effects=True, vmem_limit_bytes=56 * 1024 * 1024
        ),
        name=f"exchange_{b}",
    )(offsets, writers, tab, jnp.asarray(c2, jnp.int32), jnp.asarray(c3, jnp.int32), x0, x1, x2)


def tables_kernel(ids_ref, which_ref, tab_ref):
    i32, f32 = jnp.int32, jnp.float32
    zh = (lax.axis_index("ep") // 4) % 2

    def at(shape, d):
        return lax.broadcasted_iota(i32, shape, d)

    add = total_of
    eye = at((32, 32), 0) == at((32, 32), 1)

    def col(v):
        return add(eye, v.astype(f32), 1).astype(i32)

    ids, e = ids_ref[...], at((1, 32), 1)
    pos = add(col(ids) < ids, 1.0, 0).astype(i32)
    plane, dz, dxy = (e // 4) % 2, (pos // 4) % 2, (pos // 8) * 4 + pos % 4
    group = (plane * 2 + dz) * 16
    cg, cd = col(group), col(dxy)
    k = add((cg == group) & (cd < dxy), 1.0, 0).astype(i32)
    key = jnp.where(dz == zh, jnp.where(plane == zh, 0, 16) + k, -1)
    lane = at((32, 128), 1)
    dtab = add(col(key) == lane, (cd + 100).astype(f32), 0) - 100.0
    own = (at((32, 128), 0) == (lane // 4) * 8 + zh * 4 + lane % 4) & (lane < 16)
    kj = add(own, (col(k) * UNIT).astype(f32), 0)
    oj = add(own & (col(dz) != zh), 1.0, 0)
    r = at((8, 128), 0)
    tab_ref[...] = jnp.where(r == 0, dtab, jnp.where(r == 1, kj, jnp.where(r == 2, oj, 0.0)))
    m = jnp.sum(jnp.where((plane == 0) & (dz == 1), 1.0, 0.0)).astype(i32)
    which = jnp.int32(0)
    for _, hi in BINS[:-1]:
        which = which + jnp.where(m > hi, 1, 0)
    which_ref[0, 0] = which


def tables(expert_ids):
    vm = pl.BlockSpec(memory_space=pltpu.VMEM)
    return pl.pallas_call(
        tables_kernel,
        out_shape=(jax.ShapeDtypeStruct((1, 1), jnp.int32), jax.ShapeDtypeStruct((8, 128), jnp.float32)),
        in_specs=[vm],
        out_specs=(pl.BlockSpec(memory_space=pltpu.SMEM), vm),
        name="tables",
    )(expert_ids.reshape(1, 32))


def on_device(master_weights, first_moment, second_moment, expert_ids, bucket_offsets, writer_rank):
    which, tab = tables(expert_ids)
    saved = lax.switch(
        which[0, 0],
        [functools.partial(exchange, b) for b in range(len(BINS))],
        bucket_offsets.reshape(8, 128), writer_rank.reshape(8, 128), tab, master_weights[0], first_moment[0], second_moment[0],
    )
    return saved[:, None]


def solution(mesh):
    return jax.shard_map(
        on_device,
        mesh=mesh,
        in_specs=(P("ep", "dp", None), P("ep", "dp", None), P("ep", "dp", None), P(), P(), P()),
        out_specs=P(None, "ep", "dp", None),
        check_vma=False,
    )
```
